32 devices in a mesh: pairs: 8 (over y, x, core), aux: 4 (over z).
Axes of the slice: x: 2, y: 2, z: 4, core: 2. Of those that a mesh axis runs over, the one named last changes fastest.
Arguments:
- panels: bfloat16 [64, 3584, 256], P(None, ('pairs', 'aux')), may hold values from -0.59765625 to 0.59765625
- domain: int32 [8, 6], replicated, may hold values from 0 to 63, as said below
- pair_slots: int32 [96, 2], P('pairs'), may hold values from 0 to 5
- ranks: int32 [96, 2], P('pairs'), may hold values from 40 to 128
- transforms: bfloat16 [96, 2, 256, 128], P('pairs'), may hold values from -0.375 to 0.375
- trial: bfloat16 [96, 2, 128, 128], P('pairs'), may hold values from -0.5 to 0.5
Outputs:
- sigma: bfloat16 [96, 2, 128, 128], P('pairs', None, 'aux')
The draws below stay inside these ranges and needn't reach their ends.
Inputs may be any that keep to these rules, and one draw needn't show every extreme that they name: `domain`: each row holds 6 different LMO numbers.
All inputs are finite; a program needn't handle non-finite values.
Results may differ from the reference program's by a relative error of at most 0.0039.
Values may be sent and summed in bfloat16 or wider, within the bound.
A program may use at most 128 MiB of HBM per device.

```python
import jax
import jax.numpy as jnp
from jax import lax

NV = 256
R = 128
ROOTS = 2
NOCC = 64
LSLOT = 6
PAIR_DEV = 12
NAUX = 3584
GROUPS = 8
PAIRS = 96


def draw_domain(key, part):
    keys = jax.random.split(jax.random.fold_in(key, 11), GROUPS)
    rows = jax.vmap(lambda single: jax.random.permutation(single, NOCC)[:LSLOT])(keys)
    return rows.astype(jnp.int32)


def place_ends(drawn, stream_key, smallest, largest):
    longest = drawn.shape.index(max(drawn.shape))
    spots = []
    for shift in (0, 1):
        where = [jax.random.randint(jax.random.fold_in(stream_key, axis), (), 0, length) for axis, length in enumerate(drawn.shape)]
        where[longest] = (where[longest] + shift) % drawn.shape[longest]
        spots.append(tuple(where))
    return drawn.at[spots[0]].set(smallest).at[spots[1]].set(largest)


def steps_of(rng, shape, cuts, least, largest):
    gain, own = 1.0, jax.random.fold_in(rng, 6)
    for axis_at, parts in cuts:
        draws = jnp.exp(jax.random.uniform(jax.random.fold_in(own, axis_at), (parts,), jnp.float32, least / len(cuts), largest / len(cuts)))
        gain = gain * jnp.repeat(draws, shape[axis_at] // parts).reshape([-1 if axis == axis_at else 1 for axis in range(len(shape))])
    return gain


def normal_values(rng, extent, deviation, reach, cuts=(), held_as=jnp.bfloat16):
    values = deviation * jax.random.normal(rng, extent, jnp.float32)
    if cuts:
        values = values * steps_of(rng, extent, cuts, -0.22, 0.18)
    return jnp.clip(values, -reach, reach).astype(held_as)


def setup_inputs(seed: int = 0) -> dict:
    key_of = jax.random.split(jax.random.key(seed), 7)
    panels = normal_values(key_of[0], (NOCC, NAUX, NV), 0.08, 0.59765625, ((1, 32),))
    domain = draw_domain(jax.random.fold_in(key_of[6], 71), 0)
    pair_slots = place_ends(jax.random.randint(key_of[2], (PAIRS, 2), 0, LSLOT), jax.random.fold_in(key_of[2], 1), 0, LSLOT - 1).astype(jnp.int32)
    ranks = place_ends(jax.random.randint(key_of[3], (PAIRS, ROOTS), R * 5 // 16, R + 1), jax.random.fold_in(key_of[3], 1), R * 5 // 16, R).astype(jnp.int32)
    transforms = normal_values(key_of[4], (PAIRS, ROOTS, NV, R), NV ** -0.5, 0.375, ((0, 8),))
    trial = normal_values(key_of[5], (PAIRS, ROOTS, R, R), R ** -0.5, 0.5, ((0, 8),))
    return {"panels": panels, "domain": domain, "pair_slots": pair_slots, "ranks": ranks, "transforms": transforms, "trial": trial}


def reference(panels, domain, pair_slots, ranks, transforms, trial):
    positions = jnp.arange(R, dtype=jnp.int32)

    def one_pair(index):
        group = index // PAIR_DEV
        lmo_ids = domain[group][pair_slots[index]]
        left = panels[lmo_ids[0]].astype(jnp.float32)
        right = panels[lmo_ids[1]].astype(jnp.float32)
        keep = (positions[None, :] < ranks[index][:, None]).astype(jnp.float32)
        coeffs = transforms[index].astype(jnp.float32) * keep[:, None, :]
        amplitude = trial[index].astype(jnp.float32) * keep[:, :, None] * keep[:, None, :]
        left_proj = jnp.einsum('qv,svr->sqr', left, coeffs, precision=lax.Precision.HIGHEST).astype(jnp.bfloat16)
        right_proj = jnp.einsum('qv,svr->sqr', right, coeffs, precision=lax.Precision.HIGHEST).astype(jnp.bfloat16)
        left_proj, right_proj = lax.optimization_barrier((left_proj, right_proj))
        kmat = jnp.einsum('sqa,sqb->sab', left_proj.astype(jnp.float32), right_proj.astype(jnp.float32), precision=lax.Precision.HIGHEST)
        with_right = jnp.einsum('sab,sbc->sac', kmat, amplitude, precision=lax.Precision.HIGHEST)
        with_left = jnp.einsum('sac,sbc->sab', amplitude, kmat, precision=lax.Precision.HIGHEST)
        return (kmat + with_right + with_left).astype(jnp.bfloat16)

    return lax.map(one_pair, jnp.arange(PAIRS, dtype=jnp.int32))
```

```python
import jax
import jax.numpy as jnp
from jax import lax
from jax.experimental import pallas as pl
from jax.experimental.pallas import tpu as pltpu
from jax.sharding import PartitionSpec as P


def pair_kernel(slots_ref, ranks_ref, panels_ref, d_ref, c_ref, out_ref):
    pair = pl.program_id(0)
    left_slot = slots_ref[pair, 0]
    right_slot = slots_ref[pair, 1]
    roots = d_ref.shape[1]
    width = d_ref.shape[3]
    columns = lax.broadcasted_iota(jnp.int32, (1, width), 1)
    rows = lax.broadcasted_iota(jnp.int32, (width, 1), 0)
    masked = []
    for root in range(roots):
        rank = ranks_ref[pair, root]
        masked.append(jnp.where(columns < rank, d_ref[0, root], jnp.zeros((), d_ref.dtype)))
    coeffs = jnp.concatenate(masked, axis=1)
    left = jnp.dot(panels_ref[left_slot], coeffs, preferred_element_type=jnp.float32).astype(jnp.bfloat16)
    right = jnp.dot(panels_ref[right_slot], coeffs, preferred_element_type=jnp.float32).astype(jnp.bfloat16)
    for root in range(roots):
        rank = ranks_ref[pair, root]
        part = slice(root * width, (root + 1) * width)
        kmat = lax.dot_general(
            left[:, part], right[:, part], (((0,), (0,)), ((), ())), preferred_element_type=jnp.float32
        )
        keep = (columns < rank) & (rows < rank)
        amplitude = jnp.where(keep, c_ref[0, root], jnp.zeros((), c_ref.dtype))
        rounded = kmat.astype(jnp.bfloat16)
        with_right = jnp.dot(rounded, amplitude, preferred_element_type=jnp.float32)
        with_left = lax.dot_general(
            amplitude, rounded, (((1,), (1,)), ((), ())), preferred_element_type=jnp.float32
        )
        out_ref[0, root] = kmat + with_right + with_left


def per_device(panels, domain, pair_slots, ranks, transforms, trial):
    outgoing = panels.at[domain.reshape(-1)].get(mode="promise_in_bounds")
    received = lax.all_to_all(outgoing, "pairs", split_axis=0, concat_axis=1, tiled=True)
    pairs, roots, nv, width = transforms.shape
    slots, rows, _ = received.shape
    partial = pl.pallas_call(
        pair_kernel,
        grid=(pairs,),
        in_specs=[
            pl.BlockSpec(memory_space=pltpu.SMEM),
            pl.BlockSpec(memory_space=pltpu.SMEM),
            pl.BlockSpec((slots, rows, nv), lambda p: (0, 0, 0)),
            pl.BlockSpec((1, roots, nv, width), lambda p: (p, 0, 0, 0)),
            pl.BlockSpec((1, roots, width, width), lambda p: (p, 0, 0, 0)),
        ],
        out_specs=pl.BlockSpec((1, roots, width, width), lambda p: (p, 0, 0, 0)),
        out_shape=jax.ShapeDtypeStruct((pairs, roots, width, width), jnp.float32),
    )(pair_slots, ranks, received, transforms, trial)
    summed = lax.psum_scatter(partial, "aux", scatter_dimension=2, tiled=True)
    return summed.astype(jnp.bfloat16)


def solution(mesh):
    return jax.shard_map(
        per_device,
        mesh=mesh,
        in_specs=(
            P(None, ("pairs", "aux"), None),
            P(),
            P("pairs", None),
            P("pairs", None),
            P("pairs", None, None, None),
            P("pairs", None, None, None),
        ),
        out_specs=P("pairs", None, "aux", None),
        check_vma=False,
    )
```

```python
import functools

import jax
import jax.numpy as jnp
from jax import lax
from jax.experimental import pallas as pl
from jax.experimental.pallas import tpu as pltpu
from jax.sharding import PartitionSpec as P

MESH = pl.DeviceIdType.MESH
CHUNKS = 4


def peer_of(me, offset, count):
    if count & (count - 1):
        return lax.rem(me + offset, count)
    peer = me
    bit = 1
    while bit < count:
        if offset & bit:
            peer = peer + bit * (1 - 2 * lax.rem(me // bit, 2))
        bit *= 2
    return peer


def fused_kernel(
    n, m, lanes, slots_ref, ranks_ref, outgoing_ref, d_ref, c_ref, out_ref,
    d_raw, d_mask, c_raw, acc, send_buf, landed,
    local_sem, send_sem, recv_sem, part_send, part_recv, *received,
):
    me = lax.axis_index("pairs")
    mine = lax.axis_index("aux")
    pairs, roots, nv, width = d_ref.shape
    slots = received[0].shape[0]
    rows = received[0].shape[2]
    strip = width // m
    group = pairs // CHUNKS

    barrier = pltpu.get_barrier_semaphore()
    for offset in range(1, n):
        pl.semaphore_signal(barrier, inc=1, device_id=(peer_of(me, offset, n), mine), device_id_type=MESH)
    for offset in range(1, m):
        pl.semaphore_signal(barrier, inc=1, device_id=(me, lax.rem(mine + offset, m)), device_id_type=MESH)
    own = pltpu.make_async_copy(outgoing_ref.at[pl.ds(me * slots, slots)], received[0].at[:, 0], local_sem.at[0])
    own.start()
    d_copy = pltpu.make_async_copy(d_ref, d_raw, local_sem.at[1])
    d_copy.start()
    c_copy = pltpu.make_async_copy(c_ref, c_raw, local_sem.at[2])
    c_copy.start()
    pl.semaphore_wait(barrier, n + m - 2)

    copies = []
    for offset in range(1, n):
        peer = peer_of(me, offset, n)
        copy = pltpu.make_async_remote_copy(
            src_ref=outgoing_ref.at[pl.ds(peer * slots, slots)],
            dst_ref=received[offset // lanes].at[:, offset % lanes],
            send_sem=send_sem.at[offset],
            recv_sem=recv_sem.at[offset],
            device_id=(peer, mine),
            device_id_type=MESH,
        )
        copy.start()
        copies.append(copy)

    columns = lax.broadcasted_iota(jnp.int32, (1, width), 1)
    row_ids = lax.broadcasted_iota(jnp.int32, (width, 1), 0)
    d_copy.wait()
    c_copy.wait()

    def mask_pair(pair, carry):
        for root in range(roots):
            rank = ranks_ref[pair, root]
            d_mask[pair, :, root * width:(root + 1) * width] = jnp.where(
                columns < rank, d_raw[pair, root], jnp.zeros((), d_raw.dtype)
            )
            keep = (columns < rank) & (row_ids < rank)
            c_raw[pair, root] = jnp.where(keep, c_raw[pair, root], jnp.zeros((), c_raw.dtype))
        return carry

    lax.fori_loop(0, pairs, mask_pair, 0)

    def partial_of(pair, block):
        both = lanes * rows
        left = block[slots_ref[pair, 0]].reshape(both, nv)
        right = block[slots_ref[pair, 1]].reshape(both, nv)
        coeffs = d_mask[pair]
        left = jnp.dot(left, coeffs, preferred_element_type=jnp.float32).astype(jnp.bfloat16)
        right = jnp.dot(right, coeffs, preferred_element_type=jnp.float32).astype(jnp.bfloat16)
        return [
            lax.dot_general(
                left[:, root * width:(root + 1) * width],
                right[:, root * width:(root + 1) * width],
                (((0,), (0,)), ((), ())),
                preferred_element_type=jnp.float32,
            )
            for root in range(roots)
        ]

    stages = len(received)
    for stage in range(stages):
        for lane in range(lanes):
            offset = stage * lanes + lane
            if offset == 0:
                own.wait()
            else:
                copies[offset - 1].wait_recv()
        block = received[stage]
        if stage < stages - 1:

            def accumulate(pair, carry, block=block, stage=stage):
                parts = partial_of(pair, block)
                for root in range(roots):
                    if stage == 0:
                        acc[pair, root] = parts[root]
                    else:
                        acc[pair, root] += parts[root]
                return carry

            lax.fori_loop(0, pairs, accumulate, 0, unroll=2)

    block = received[stages - 1]

    def finish(pair, carry):
        parts = partial_of(pair, block)
        for root in range(roots):
            kmat = parts[root] if stages == 1 else acc[pair, root] + parts[root]
            rounded = kmat.astype(jnp.bfloat16)
            amplitude = c_raw[pair, root]
            with_right = jnp.dot(rounded, amplitude, preferred_element_type=jnp.float32)
            with_left = lax.dot_general(
                amplitude, rounded, (((1,), (1,)), ((), ())), preferred_element_type=jnp.float32
            )
            sigma = kmat + with_right + with_left
            acc[pair, root] = sigma
            for owner in range(m):
                send_buf[owner, pair, root] = sigma[owner * strip:(owner + 1) * strip].astype(jnp.bfloat16)
        return carry

    sums = []
    for chunk in range(CHUNKS):
        lax.fori_loop(chunk * group, (chunk + 1) * group, finish, 0, unroll=group)
        for offset in range(1, m):
            peer = lax.rem(mine + offset, m)
            copy = pltpu.make_async_remote_copy(
                src_ref=send_buf.at[peer, pl.ds(chunk * group, group)],
                dst_ref=landed.at[offset - 1, pl.ds(chunk * group, group)],
                send_sem=part_send.at[chunk, offset],
                recv_sem=part_recv.at[chunk, offset],
                device_id=(me, peer),
                device_id_type=MESH,
            )
            copy.start()
            sums.append((chunk, offset, copy))

    for chunk in range(CHUNKS):
        for at, offset, copy in sums:
            if at == chunk:
                copy.wait_recv()
        part = pl.ds(chunk * group, group)
        total = acc[part, :, pl.ds(mine * strip, strip), :]
        for offset in range(1, m):
            total = total + landed[offset - 1, part].astype(jnp.float32)
        out_ref[part] = total.astype(out_ref.dtype)
    for copy in copies:
        copy.wait_send()
    for _, _, copy in sums:
        copy.wait_send()


def per_device(n, m, panels, domain, pair_slots, ranks, transforms, trial):
    pairs, roots, nv, width = transforms.shape
    slots = domain.shape[1]
    rows = panels.shape[1]
    lanes = 2
    outgoing = panels.at[domain.reshape(-1)].get(mode="promise_in_bounds")
    smem = pl.BlockSpec(memory_space=pltpu.SMEM)
    hbm = pl.BlockSpec(memory_space=pltpu.HBM)
    return pl.pallas_call(
        functools.partial(fused_kernel, n, m, lanes),
        in_specs=[smem, smem, hbm, hbm, hbm],
        out_specs=pl.BlockSpec(memory_space=pltpu.VMEM),
        out_shape=jax.ShapeDtypeStruct((pairs, roots, width // m, width), jnp.bfloat16),
        scratch_shapes=[
            pltpu.VMEM((pairs, roots, nv, width), transforms.dtype),
            pltpu.VMEM((pairs, nv, roots * width), transforms.dtype),
            pltpu.VMEM((pairs, roots, width, width), trial.dtype),
            pltpu.VMEM((pairs, roots, width, width), jnp.float32),
            pltpu.VMEM((m, pairs, roots, width // m, width), jnp.bfloat16),
            pltpu.VMEM((m - 1, pairs, roots, width // m, width), jnp.bfloat16),
            pltpu.SemaphoreType.DMA((3,)),
            pltpu.SemaphoreType.DMA((n,)),
            pltpu.SemaphoreType.DMA((n,)),
            pltpu.SemaphoreType.DMA((CHUNKS, m)),
            pltpu.SemaphoreType.DMA((CHUNKS, m)),
        ]
        + [pltpu.VMEM((slots, lanes, rows, nv), panels.dtype) for _ in range(n // lanes)],
        compiler_params=pltpu.CompilerParams(
            collective_id=0, has_side_effects=True, vmem_limit_bytes=60 * 2**20
        ),
    )(pair_slots, ranks, outgoing, transforms, trial)


def solution(mesh):
    return jax.shard_map(
        functools.partial(per_device, mesh.shape["pairs"], mesh.shape["aux"]),
        mesh=mesh,
        in_specs=(
            P(None, ("pairs", "aux"), None),
            P(),
            P("pairs", None),
            P("pairs", None),
            P("pairs", None, None, None),
            P("pairs", None, None, None),
        ),
        out_specs=P("pairs", None, "aux", None),
        check_vma=False,
    )
```

```python
import functools

import jax
import jax.numpy as jnp
from jax import lax
from jax.experimental import pallas as pl
from jax.experimental.pallas import tpu as pltpu
from jax.sharding import PartitionSpec as P

MESH = pl.DeviceIdType.MESH
CHUNKS = 4


def peer_of(me, offset, count):
    if count & (count - 1):
        return lax.rem(me + offset, count)
    peer = me
    bit = 1
    while bit < count:
        if offset & bit:
            peer = peer + bit * (1 - 2 * lax.rem(me // bit, 2))
        bit *= 2
    return peer


def fused_kernel(
    n, m, plan, domain_ref, slots_ref, ranks_ref, panels_ref, d_ref, c_ref, out_ref,
    panels, outgoing, d_raw, d_mask, c_raw, acc, send_buf, landed,
    local_sem, send_sem, recv_sem, part_send, part_recv, *received,
):
    me = lax.axis_index("pairs")
    mine = lax.axis_index("aux")
    pairs, roots, nv, width = d_ref.shape
    slots = received[0].shape[0]
    rows = received[0].shape[2]
    strip = width // m
    group = pairs // CHUNKS

    barrier = pltpu.get_barrier_semaphore()
    for offset in range(1, n):
        pl.semaphore_signal(barrier, inc=1, device_id=(peer_of(me, offset, n), mine), device_id_type=MESH)
    for offset in range(1, m):
        pl.semaphore_signal(barrier, inc=1, device_id=(me, lax.rem(mine + offset, m)), device_id_type=MESH)
    panels_copy = pltpu.make_async_copy(panels_ref, panels, local_sem.at[0])
    panels_copy.start()
    d_copy = pltpu.make_async_copy(d_ref, d_raw, local_sem.at[1])
    d_copy.start()
    c_copy = pltpu.make_async_copy(c_ref, c_raw, local_sem.at[2])
    c_copy.start()
    pl.semaphore_wait(barrier, n + m - 2)

    panels_copy.wait()
    place = {offset: (stage, lane) for stage, group in enumerate(plan) for lane, offset in enumerate(group)}
    copies = {}
    for offset in range(1, n):
        peer = peer_of(me, offset, n)
        for slot in range(slots):
            outgoing[offset - 1, slot] = panels[domain_ref[peer, slot]]
        stage, lane = place[offset]
        copies[offset] = pltpu.make_async_remote_copy(
            src_ref=outgoing.at[offset - 1],
            dst_ref=received[stage].at[:, lane],
            send_sem=send_sem.at[offset],
            recv_sem=recv_sem.at[offset],
            device_id=(peer, mine),
            device_id_type=MESH,
        )
        if offset > 1:
            copies[offset - 1].start()
    for slot in range(slots):
        received[0][slot, 0] = panels[domain_ref[me, slot]]
    copies[n - 1].start()

    columns = lax.broadcasted_iota(jnp.int32, (1, width), 1)
    row_ids = lax.broadcasted_iota(jnp.int32, (width, 1), 0)
    d_copy.wait()
    c_copy.wait()

    def mask_pair(pair, carry):
        for root in range(roots):
            rank = ranks_ref[root, pair]
            d_mask[pair, :, root * width:(root + 1) * width] = jnp.where(
                columns < rank, d_raw[pair, root], jnp.zeros((), d_raw.dtype)
            )
            keep = (columns < rank) & (row_ids < rank)
            c_raw[pair, root] = jnp.where(keep, c_raw[pair, root], jnp.zeros((), c_raw.dtype))
        return carry

    lax.fori_loop(0, pairs, mask_pair, 0)

    def partial_of(pair, block):
        both = block.shape[1] * rows
        left = block[slots_ref[0, pair]].reshape(both, nv)
        right = block[slots_ref[1, pair]].reshape(both, nv)
        coeffs = d_mask[pair]
        left = jnp.dot(left, coeffs, preferred_element_type=jnp.float32).astype(jnp.bfloat16)
        right = jnp.dot(right, coeffs, preferred_element_type=jnp.float32).astype(jnp.bfloat16)
        return [
            lax.dot_general(
                left[:, root * width:(root + 1) * width],
                right[:, root * width:(root + 1) * width],
                (((0,), (0,)), ((), ())),
                preferred_element_type=jnp.float32,
            )
            for root in range(roots)
        ]

    stages = len(received)
    for stage in range(stages):
        for offset in plan[stage]:
            if offset:
                copies[offset].wait_recv()
        block = received[stage]
        if stage < stages - 1:

            def accumulate(pair, carry, block=block, stage=stage):
                parts = partial_of(pair, block)
                for root in range(roots):
                    if stage == 0:
                        acc[pair, root] = parts[root]
                    else:
                        acc[pair, root] += parts[root]
                return carry

            lax.fori_loop(0, pairs, accumulate, 0, unroll=2)

    block = received[stages - 1]

    def finish(pair, carry):
        parts = partial_of(pair, block)
        for root in range(roots):
            kmat = parts[root] if stages == 1 else acc[pair, root] + parts[root]
            rounded = kmat.astype(jnp.bfloat16)
            amplitude = c_raw[pair, root]
            with_right = jnp.dot(rounded, amplitude, preferred_element_type=jnp.float32)
            with_left = lax.dot_general(
                amplitude, rounded, (((1,), (1,)), ((), ())), preferred_element_type=jnp.float32
            )
            sigma = kmat + with_right + with_left
            acc[pair, root] = sigma
            for owner in range(m):
                send_buf[owner, pair, root] = sigma[owner * strip:(owner + 1) * strip].astype(jnp.bfloat16)
        return carry

    sums = []
    for chunk in range(CHUNKS):
        lax.fori_loop(chunk * group, (chunk + 1) * group, finish, 0, unroll=group)
        for offset in range(1, m):
            peer = lax.rem(mine + offset, m)
            copy = pltpu.make_async_remote_copy(
                src_ref=send_buf.at[peer, pl.ds(chunk * group, group)],
                dst_ref=landed.at[offset - 1, pl.ds(chunk * group, group)],
                send_sem=part_send.at[chunk, offset],
                recv_sem=part_recv.at[chunk, offset],
                device_id=(me, peer),
                device_id_type=MESH,
            )
            copy.start()
            sums.append((chunk, offset, copy))

    for chunk in range(CHUNKS):
        for at, offset, copy in sums:
            if at == chunk:
                copy.wait_recv()
        part = pl.ds(chunk * group, group)
        total = acc[part, :, pl.ds(mine * strip, strip), :]
        for offset in range(1, m):
            total = total + landed[offset - 1, part].astype(jnp.float32)
        out_ref[part] = total.astype(out_ref.dtype)
    for copy in copies.values():
        copy.wait_send()
    for _, _, copy in sums:
        copy.wait_send()


def per_device(n, m, panels, domain, pair_slots, ranks, transforms, trial):
    pairs, roots, nv, width = transforms.shape
    slots = domain.shape[1]
    rows = panels.shape[1]
    plan = [(offset, offset + 1) for offset in range(0, n - 2, 2)] + [(n - 2,), (n - 1,)]
    smem = pl.BlockSpec(memory_space=pltpu.SMEM)
    hbm = pl.BlockSpec(memory_space=pltpu.HBM)
    return pl.pallas_call(
        functools.partial(fused_kernel, n, m, plan),
        in_specs=[smem, smem, smem, hbm, hbm, hbm],
        out_specs=pl.BlockSpec(memory_space=pltpu.VMEM),
        out_shape=jax.ShapeDtypeStruct((pairs, roots, width // m, width), jnp.bfloat16),
        scratch_shapes=[
            pltpu.VMEM(panels.shape, panels.dtype),
            pltpu.VMEM((n - 1, slots, rows, nv), panels.dtype),
            pltpu.VMEM((pairs, roots, nv, width), transforms.dtype),
            pltpu.VMEM((pairs, nv, roots * width), transforms.dtype),
            pltpu.VMEM((pairs, roots, width, width), trial.dtype),
            pltpu.VMEM((pairs, roots, width, width), jnp.float32),
            pltpu.VMEM((m, pairs, roots, width // m, width), jnp.bfloat16),
            pltpu.VMEM((m - 1, pairs, roots, width // m, width), jnp.bfloat16),
            pltpu.SemaphoreType.DMA((3,)),
            pltpu.SemaphoreType.DMA((n,)),
            pltpu.SemaphoreType.DMA((n,)),
            pltpu.SemaphoreType.DMA((CHUNKS, m)),
            pltpu.SemaphoreType.DMA((CHUNKS, m)),
        ]
        + [pltpu.VMEM((slots, len(group), rows, nv), panels.dtype) for group in plan],
        compiler_params=pltpu.CompilerParams(
            collective_id=0, has_side_effects=True, vmem_limit_bytes=60 * 2**20
        ),
    )(domain, pair_slots.T, ranks.T, panels, transforms, trial)


def solution(mesh):
    return jax.shard_map(
        functools.partial(per_device, mesh.shape["pairs"], mesh.shape["aux"]),
        mesh=mesh,
        in_specs=(
            P(None, ("pairs", "aux"), None),
            P(),
            P("pairs", None),
            P("pairs", None),
            P("pairs", None, None, None),
            P("pairs", None, None, None),
        ),
        out_specs=P("pairs", None, "aux", None),
        check_vma=False,
    )
```

```python
import functools

import jax
import jax.numpy as jnp
from jax import lax
from jax.experimental import pallas as pl
from jax.experimental.pallas import tpu as pltpu
from jax.sharding import PartitionSpec as P

MESH = pl.DeviceIdType.MESH
CHUNKS = 6


def peer_of(me, offset, count):
    if count & (count - 1):
        return lax.rem(me + offset, count)
    peer = me
    bit = 1
    while bit < count:
        if offset & bit:
            peer = peer + bit * (1 - 2 * lax.rem(me // bit, 2))
        bit *= 2
    return peer


def fused_kernel(
    n, m, plan, domain_ref, slots_ref, ranks_ref, panels_ref, d_ref, c_ref, out_ref,
    panels, outgoing, d_raw, d_mask, c_raw, acc, send_buf, landed,
    local_sem, send_sem, recv_sem, part_send, part_recv, *received,
):
    me = lax.axis_index("pairs")
    mine = lax.axis_index("aux")
    pairs, roots, nv, width = d_ref.shape
    slots = received[0].shape[0]
    rows = received[0].shape[2]
    strip = width // m
    group = pairs // CHUNKS

    barrier = pltpu.get_barrier_semaphore()
    for offset in range(1, n):
        pl.semaphore_signal(barrier, inc=1, device_id=(peer_of(me, offset, n), mine), device_id_type=MESH)
    for offset in range(1, m):
        pl.semaphore_signal(barrier, inc=1, device_id=(me, lax.rem(mine + offset, m)), device_id_type=MESH)
    panels_copy = pltpu.make_async_copy(panels_ref, panels, local_sem.at[0])
    panels_copy.start()
    d_copy = pltpu.make_async_copy(d_ref, d_raw, local_sem.at[1])
    d_copy.start()
    c_copy = pltpu.make_async_copy(c_ref, c_raw, local_sem.at[2])
    c_copy.start()
    pl.semaphore_wait(barrier, n + m - 2)

    panels_copy.wait()
    place = {offset: (stage, lane) for stage, group in enumerate(plan) for lane, offset in enumerate(group)}
    copies = {}
    for offset in range(1, n):
        peer = peer_of(me, offset, n)
        for slot in range(slots):
            outgoing[offset - 1, slot] = panels[domain_ref[peer, slot]]
        stage, lane = place[offset]
        copies[offset] = pltpu.make_async_remote_copy(
            src_ref=outgoing.at[offset - 1],
            dst_ref=received[stage].at[:, lane],
            send_sem=send_sem.at[offset],
            recv_sem=recv_sem.at[offset],
            device_id=(peer, mine),
            device_id_type=MESH,
        )
        if offset > 1:
            copies[offset - 1].start()
    for slot in range(slots):
        received[0][slot, 0] = panels[domain_ref[me, slot]]
    copies[n - 1].start()

    columns = lax.broadcasted_iota(jnp.int32, (1, width), 1)
    row_ids = lax.broadcasted_iota(jnp.int32, (width, 1), 0)
    d_copy.wait()
    c_copy.wait()

    def mask_pair(pair, carry):
        for root in range(roots):
            rank = ranks_ref[root, pair]
            d_mask[pair, :, root * width:(root + 1) * width] = jnp.where(
                columns < rank, d_raw[pair, root], jnp.zeros((), d_raw.dtype)
            )
            keep = (columns < rank) & (row_ids < rank)
            c_raw[pair, root] = jnp.where(keep, c_raw[pair, root], jnp.zeros((), c_raw.dtype))
        return carry

    lax.fori_loop(0, pairs, mask_pair, 0)

    def partial_of(pair, block):
        both = block.shape[1] * rows
        left = block[slots_ref[0, pair]].reshape(both, nv)
        right = block[slots_ref[1, pair]].reshape(both, nv)
        coeffs = d_mask[pair]
        left = jnp.dot(left, coeffs, preferred_element_type=jnp.float32).astype(jnp.bfloat16)
        right = jnp.dot(right, coeffs, preferred_element_type=jnp.float32).astype(jnp.bfloat16)
        return [
            lax.dot_general(
                left[:, root * width:(root + 1) * width],
                right[:, root * width:(root + 1) * width],
                (((0,), (0,)), ((), ())),
                preferred_element_type=jnp.float32,
            )
            for root in range(roots)
        ]

    stages = len(received)
    for stage in range(stages):
        for offset in plan[stage]:
            if offset:
                copies[offset].wait_recv()
        block = received[stage]
        if stage < stages - 1:

            def accumulate(pair, carry, block=block, stage=stage):
                parts = partial_of(pair, block)
                for root in range(roots):
                    if stage == 0:
                        acc[pair, root] = parts[root]
                    else:
                        acc[pair, root] += parts[root]
                return carry

            lax.fori_loop(0, pairs, accumulate, 0, unroll=2)

    block = received[stages - 1]

    def finish(pair, carry):
        parts = partial_of(pair, block)
        for root in range(roots):
            kmat = parts[root] if stages == 1 else acc[pair, root] + parts[root]
            rounded = kmat.astype(jnp.bfloat16)
            amplitude = c_raw[pair, root]
            with_right = jnp.dot(rounded, amplitude, preferred_element_type=jnp.float32)
            with_left = lax.dot_general(
                amplitude, rounded, (((1,), (1,)), ((), ())), preferred_element_type=jnp.float32
            )
            sigma = kmat + with_right + with_left
            acc[pair, root] = sigma
            for owner in range(m):
                send_buf[owner, pair, root] = sigma[owner * strip:(owner + 1) * strip].astype(jnp.bfloat16)
        return carry

    sums = []
    for chunk in range(CHUNKS):
        lax.fori_loop(chunk * group, (chunk + 1) * group, finish, 0, unroll=group)
        for offset in sorted(range(1, m), key=lambda hop: -min(hop, m - hop)):
            peer = lax.rem(mine + offset, m)
            copy = pltpu.make_async_remote_copy(
                src_ref=send_buf.at[peer, pl.ds(chunk * group, group)],
                dst_ref=landed.at[offset - 1, pl.ds(chunk * group, group)],
                send_sem=part_send.at[chunk, offset],
                recv_sem=part_recv.at[chunk, offset],
                device_id=(me, peer),
                device_id_type=MESH,
            )
            copy.start()
            sums.append((chunk, offset, copy))

    for chunk in range(CHUNKS):
        for at, offset, copy in sums:
            if at == chunk:
                copy.wait_recv()
        part = pl.ds(chunk * group, group)
        total = acc[part, :, pl.ds(mine * strip, strip), :]
        for offset in range(1, m):
            total = total + landed[offset - 1, part].astype(jnp.float32)
        out_ref[part] = total.astype(out_ref.dtype)
    for copy in copies.values():
        copy.wait_send()
    for _, _, copy in sums:
        copy.wait_send()


def per_device(n, m, panels, domain, pair_slots, ranks, transforms, trial):
    pairs, roots, nv, width = transforms.shape
    slots = domain.shape[1]
    rows = panels.shape[1]
    plan = [(offset, offset + 1) for offset in range(0, n - 2, 2)] + [(n - 2,), (n - 1,)]
    smem = pl.BlockSpec(memory_space=pltpu.SMEM)
    hbm = pl.BlockSpec(memory_space=pltpu.HBM)
    return pl.pallas_call(
        functools.partial(fused_kernel, n, m, plan),
        in_specs=[smem, smem, smem, hbm, hbm, hbm],
        out_specs=pl.BlockSpec(memory_space=pltpu.VMEM),
        out_shape=jax.ShapeDtypeStruct((pairs, roots, width // m, width), jnp.bfloat16),
        scratch_shapes=[
            pltpu.VMEM(panels.shape, panels.dtype),
            pltpu.VMEM((n - 1, slots, rows, nv), panels.dtype),
            pltpu.VMEM((pairs, roots, nv, width), transforms.dtype),
            pltpu.VMEM((pairs, nv, roots * width), transforms.dtype),
            pltpu.VMEM((pairs, roots, width, width), trial.dtype),
            pltpu.VMEM((pairs, roots, width, width), jnp.float32),
            pltpu.VMEM((m, pairs, roots, width // m, width), jnp.bfloat16),
            pltpu.VMEM((m - 1, pairs, roots, width // m, width), jnp.bfloat16),
            pltpu.SemaphoreType.DMA((3,)),
            pltpu.SemaphoreType.DMA((n,)),
            pltpu.SemaphoreType.DMA((n,)),
            pltpu.SemaphoreType.DMA((CHUNKS, m)),
            pltpu.SemaphoreType.DMA((CHUNKS, m)),
        ]
        + [pltpu.VMEM((slots, len(group), rows, nv), panels.dtype) for group in plan],
        compiler_params=pltpu.CompilerParams(
            collective_id=0, has_side_effects=True, vmem_limit_bytes=60 * 2**20
        ),
    )(domain, pair_slots.T, ranks.T, panels, transforms, trial)


def solution(mesh):
    return jax.shard_map(
        functools.partial(per_device, mesh.shape["pairs"], mesh.shape["aux"]),
        mesh=mesh,
        in_specs=(
            P(None, ("pairs", "aux"), None),
            P(),
            P("pairs", None),
            P("pairs", None),
            P("pairs", None, None, None),
            P("pairs", None, None, None),
        ),
        out_specs=P("pairs", None, "aux", None),
        check_vma=False,
    )
```
